32 devices in a mesh: dp: 2 (over x), b: 4 (over z), cp: 4 (over y, core).
Axes of the slice: x: 2, y: 2, z: 4, core: 2. Of those that a mesh axis runs over, the one named last changes fastest.
Arguments:
- x: bfloat16 [8, 4096, 2048], P(('dp', 'b'), 'cp'), parts along dimension 0
- ids: int32 [8, 4096, 6], P(('dp', 'b'), 'cp'), parts along dimension 0
- g_attn: bfloat16 [2048], replicated
- w_q: bfloat16 [2048, 3072], replicated
- w_dkv: bfloat16 [2048, 512], replicated
- w_kr: bfloat16 [2048, 64], replicated
- w_uk: bfloat16 [16, 128, 512], replicated
- w_uv: bfloat16 [16, 512, 128], replicated
- w_o: bfloat16 [2048, 2048], replicated
- g_ffn: bfloat16 [2048], replicated
- w_fg: bfloat16 [2048, 11264], replicated
- w_fu: bfloat16 [2048, 11264], replicated
- w_fd: bfloat16 [11264, 2048], replicated
- g_moe: bfloat16 [2048], replicated
- w_r: bfloat16 [2048, 96], replicated
- w_eg: bfloat16 [64, 2048, 1408], P(('b', 'cp'))
- w_eu: bfloat16 [64, 2048, 1408], P(('b', 'cp'))
- w_ed: bfloat16 [64, 1408, 2048], P(('b', 'cp'))
Outputs:
- output: bfloat16 [8, 4096, 2048], P(('dp', 'b'), 'cp'), parts along dimension 0
There are 2 independent parts. The reference program is written for one: setup_inputs(seed, part) draws one part's arguments, and reference() takes and returns one part's arrays. A program takes and returns all parts, laid end to end along the dimension named above; an argument that names none is the same for every part.
All inputs are finite; a program needn't handle non-finite values.
Results may differ from the reference program's by a relative error of at most 0.00887259.
Values are sent between devices in bfloat16 or wider.
A program may use at most 1 GiB of HBM per device.

```python
import jax
import jax.numpy as jnp
from jax import lax

D = 2048
HEADS = 16
R = 512
EXPERTS = 64
TOP = 6
EFF = 1408
FF = 11264
ROWS = 1
SEQ = 1024
NB = 4
NC = 4
NOPE = 128
ROPE = 64
VDIM = 128

B = ROWS * NB
S = SEQ * NC
T = B * S
TBLK = ROWS * SEQ
NSLOT = EXPERTS + EXPERTS // 2
WIDTH = NSLOT // TOP
HOT = WIDTH // 2
CAP = (TBLK + HOT - 1) // HOT
CAPALL = NB * NC * CAP
EPS = 1e-6
SCALE = (NOPE + ROPE) ** -0.5


def _nrm(k, shape, scale):
    return (jax.random.normal(k, shape, jnp.float32) * scale).astype(jnp.bfloat16)


def _gain(k):
    return jax.random.uniform(k, (D,), jnp.float32, 0.6, 1.4).astype(jnp.bfloat16)


def setup_inputs(seed: int = 0, part: int = 0) -> dict:
    kp = jax.random.fold_in(jax.random.key(seed), part)
    kw = jax.random.split(jax.random.key(seed + 1), 16)
    k1, k2, k3, k4, k5 = jax.random.split(kp, 5)
    pos = jnp.arange(S, dtype=jnp.float32) / S
    amp = jax.random.normal(k2, (B, 3, D), jnp.float32) * 0.6
    phase = jax.random.uniform(k3, (B, 3, 1), jnp.float32, 0.0, 6.2832)
    freq = jnp.arange(1, 4, dtype=jnp.float32).reshape(1, 3, 1)
    wave = jnp.cos(6.2832 * freq * pos.reshape(1, 1, S) + phase)
    x = 0.7 * jax.random.normal(k1, (B, S, D), jnp.float32) + jnp.einsum('clt,cle->cte', wave, amp)
    ka, kb, kc = jax.random.split(jax.random.fold_in(kp, 7), 3)
    shift = jax.random.randint(ka, (), 0, NSLOT)
    perm = (jnp.arange(NSLOT) + shift) % NSLOT
    tperm = jax.vmap(lambda kk: jax.random.permutation(kk, TBLK))(jax.random.split(kb, NB * NC * TOP))
    off = jax.random.randint(kc, (NB * NC * TOP, 1), 0, WIDTH - HOT + 1)
    r = (tperm % HOT + off).reshape(NB, NC, TOP, TBLK)
    slot = jnp.arange(TOP).reshape(1, 1, TOP, 1) * WIDTH + r
    ids = perm[slot].reshape(NB, NC, TOP, ROWS, SEQ).transpose(0, 3, 1, 4, 2).reshape(B, S, TOP)
    return {
        'x': x.astype(jnp.bfloat16),
        'ids': ids.astype(jnp.int32),
        'g_attn': _gain(kw[0]),
        'w_q': _nrm(kw[1], (D, HEADS * (NOPE + ROPE)), D ** -0.5),
        'w_dkv': _nrm(kw[2], (D, R), D ** -0.5),
        'w_kr': _nrm(kw[3], (D, ROPE), D ** -0.5),
        'w_uk': _nrm(kw[4], (HEADS, NOPE, R), 0.5 * NOPE ** -0.5),
        'w_uv': _nrm(kw[5], (HEADS, R, VDIM), R ** -0.5),
        'w_o': _nrm(kw[6], (HEADS * VDIM, D), (HEADS * VDIM) ** -0.5),
        'g_ffn': _gain(kw[7]),
        'w_fg': _nrm(kw[8], (D, FF), D ** -0.5),
        'w_fu': _nrm(kw[9], (D, FF), D ** -0.5),
        'w_fd': _nrm(kw[10], (FF, D), FF ** -0.5),
        'g_moe': _gain(kw[11]),
        'w_r': _nrm(kw[12], (D, NSLOT), 2.0 * D ** -0.5),
        'w_eg': _nrm(kw[13], (EXPERTS, D, EFF), D ** -0.5),
        'w_eu': _nrm(kw[14], (EXPERTS, D, EFF), D ** -0.5),
        'w_ed': _nrm(kw[15], (EXPERTS, EFF, D), 2.0 * EFF ** -0.5),
    }


def _rms(v, g):
    vf = v.astype(jnp.float32)
    return (vf * lax.rsqrt(jnp.mean(vf * vf, axis=-1, keepdims=True) + EPS) * g.astype(jnp.float32)).astype(jnp.bfloat16)


def _rope(v, cos, sin):
    half = ROPE // 2
    v1 = v[..., :half]
    v2 = v[..., half:]
    return jnp.concatenate([v1 * cos - v2 * sin, v1 * sin + v2 * cos], axis=-1)


def _swiglu(z, wg, wu, wd):
    hid = jax.nn.silu(jnp.dot(z, wg, preferred_element_type=jnp.float32)) * jnp.dot(z, wu, preferred_element_type=jnp.float32)
    return jnp.dot(hid.astype(jnp.bfloat16), wd, preferred_element_type=jnp.float32).astype(jnp.bfloat16)


def reference(x, ids, g_attn, w_q, w_dkv, w_kr, w_uk, w_uv, w_o, g_ffn, w_fg, w_fu, w_fd, g_moe, w_r, w_eg, w_eu, w_ed):
    pos = jnp.arange(S)
    half = ROPE // 2
    ang = pos.astype(jnp.float32)[:, None] * (10000.0 ** (-jnp.arange(half, dtype=jnp.float32) / half))[None, :]
    cos = jnp.cos(ang)
    sin = jnp.sin(ang)
    causal = pos[:, None] >= pos[None, :]

    def attn_row(xr):
        n = _rms(xr, g_attn)
        c = jnp.dot(n, w_dkv, preferred_element_type=jnp.float32).astype(jnp.bfloat16)
        kr = _rope(jnp.dot(n, w_kr, preferred_element_type=jnp.float32), cos, sin).astype(jnp.bfloat16)
        q = jnp.dot(n, w_q, preferred_element_type=jnp.float32).reshape(S, HEADS, NOPE + ROPE)
        qn = q[..., :NOPE].astype(jnp.bfloat16)
        qt = jnp.einsum('shn,hnr->shr', qn.astype(jnp.float32), w_uk.astype(jnp.float32)).astype(jnp.bfloat16)
        qr = _rope(q[..., NOPE:], cos[:, None, :], sin[:, None, :]).astype(jnp.bfloat16)

        def head(hargs):
            qh, qrh, wuv = hargs
            sc = (jnp.dot(qh, c.T, preferred_element_type=jnp.float32) + jnp.dot(qrh, kr.T, preferred_element_type=jnp.float32)) * SCALE
            sc = jnp.where(causal, sc, -jnp.inf)
            p = jnp.exp(sc - jnp.max(sc, axis=-1, keepdims=True))
            lat = (jnp.dot(p.astype(jnp.bfloat16), c, preferred_element_type=jnp.float32) / jnp.sum(p, axis=-1, keepdims=True)).astype(jnp.bfloat16)
            return jnp.dot(lat, wuv, preferred_element_type=jnp.float32).astype(jnp.bfloat16)

        o = lax.map(head, (jnp.transpose(qt, (1, 0, 2)), jnp.transpose(qr, (1, 0, 2)), w_uv))
        o = jnp.transpose(o, (1, 0, 2)).reshape(S, HEADS * VDIM)
        return jnp.dot(o, w_o, preferred_element_type=jnp.float32).astype(jnp.bfloat16)

    a = lax.map(attn_row, x)
    y = (x.astype(jnp.float32) + a.astype(jnp.float32)).astype(jnp.bfloat16)
    n2 = _rms(y, g_ffn).reshape(B * NC, SEQ, D)
    f = lax.map(lambda z: _swiglu(z, w_fg, w_fu, w_fd), n2).reshape(T, D)
    u = _rms(x, g_moe).reshape(T, D)
    idf = ids.reshape(T, TOP)
    g = jax.nn.softmax(jnp.dot(u, w_r, preferred_element_type=jnp.float32), axis=-1)
    sel = jnp.take_along_axis(g, idf, axis=1)
    gate = sel / jnp.sum(sel, axis=1, keepdims=True)
    gflat = gate.reshape(-1)
    flat = idf.reshape(-1)
    order = jnp.argsort(flat, stable=True)
    starts = jnp.searchsorted(flat[order], jnp.arange(EXPERTS + 1, dtype=flat.dtype))
    zero = jnp.sum(jnp.where(idf >= EXPERTS, gate, 0.0), axis=1)
    m0 = zero[:, None] * u.astype(jnp.float32)

    def expert(m, eargs):
        e, wg, wu, wd = eargs
        k = starts[e] + jnp.arange(CAPALL)
        slot = order[jnp.minimum(k, T * TOP - 1)]
        tok = slot // TOP
        out = _swiglu(u[tok], wg, wu, wd)
        w = jnp.where(k < starts[e + 1], gflat[slot], 0.0)
        return m.at[tok].add(w[:, None] * out.astype(jnp.float32)), None

    m, _ = lax.scan(expert, m0, (jnp.arange(EXPERTS), w_eg, w_eu, w_ed))
    h = y.reshape(T, D).astype(jnp.float32) + f.astype(jnp.float32) + m
    return h.astype(jnp.bfloat16).reshape(B, S, D)
```

```python
import functools

import jax
import jax.numpy as jnp
from jax import lax
from jax.experimental import pallas as pl
from jax.experimental.pallas import tpu as pltpu
from jax.sharding import PartitionSpec as P

NOPE = 128
ROPE = 64
EPS = 1e-6
SCALE = (NOPE + ROPE) ** -0.5
F32 = jnp.float32
BF16 = jnp.bfloat16


def _rms(v, g):
    vf = v.astype(F32)
    return (vf * lax.rsqrt(jnp.mean(vf * vf, axis=-1, keepdims=True) + EPS) * g.astype(F32)).astype(BF16)


def _rope(v, cos, sin):
    half = ROPE // 2
    v1 = v[..., :half]
    v2 = v[..., half:]
    return jnp.concatenate([v1 * cos - v2 * sin, v1 * sin + v2 * cos], axis=-1)


def _swiglu(z, wg, wu, wd):
    hid = jax.nn.silu(jnp.dot(z, wg, preferred_element_type=F32)) * jnp.dot(z, wu, preferred_element_type=F32)
    return jnp.dot(hid.astype(BF16), wd, preferred_element_type=F32).astype(BF16)


def _prep(x, pos, g_attn, w_q, w_dkv, w_kr, w_uk):
    rows, seq, _ = x.shape
    heads = w_uk.shape[0]
    half = ROPE // 2
    ang = pos.astype(F32)[:, None] * (10000.0 ** (-jnp.arange(half, dtype=F32) / half))[None, :]
    cos = jnp.cos(ang)
    sin = jnp.sin(ang)
    n = _rms(x, g_attn)
    c = jnp.einsum('bsd,dr->bsr', n, w_dkv, preferred_element_type=F32).astype(BF16)
    kr = _rope(jnp.einsum('bsd,de->bse', n, w_kr, preferred_element_type=F32), cos, sin).astype(BF16)
    q = jnp.einsum('bsd,dk->bsk', n, w_q, preferred_element_type=F32).reshape(rows, seq, heads, NOPE + ROPE)
    qt = jnp.einsum('bshn,hnr->bhsr', q[..., :NOPE].astype(BF16), w_uk, preferred_element_type=F32).astype(BF16)
    qr = _rope(jnp.transpose(q[..., NOPE:], (0, 2, 1, 3)), cos, sin).astype(BF16)
    return jnp.concatenate([qt, qr], axis=-1), jnp.concatenate([c, kr], axis=-1)


LANES = 128


def _block_kernel(r, sub, first, q_ref, kv_ref, *refs):
    if first:
        mo_ref, lo_ref, ao_ref = refs
    else:
        m_ref, l_ref, a_ref, mo_ref, lo_ref, ao_ref = refs
    kv = kv_ref[0]
    tq = q_ref.shape[1]
    for n in range(tq // sub):
        rows = pl.ds(n * sub, sub)
        sc = lax.dot_general(q_ref[0, rows, :], kv, (((1,), (1,)), ((), ())), preferred_element_type=F32) * SCALE
        if first:
            at = pl.program_id(1) * tq + n * sub
            row = at + lax.broadcasted_iota(jnp.int32, sc.shape, 0)
            col = lax.broadcasted_iota(jnp.int32, sc.shape, 1)
            sc = jnp.where(row >= col, sc, -jnp.inf)
        new = jnp.max(sc, axis=-1, keepdims=True)
        if not first:
            old = m_ref[0, rows, :1]
            new = jnp.maximum(new, old)
            corr = jnp.exp(old - new)
        p = jnp.exp(sc - new)
        den = jnp.sum(p, axis=-1, keepdims=True)
        pv = jnp.dot(p.astype(BF16), kv[:, :r], preferred_element_type=F32)
        if not first:
            den = den + l_ref[0, rows, :1] * corr
            pv = pv + a_ref[0, rows, :] * corr
        mo_ref[0, rows, :] = jnp.broadcast_to(new, (sub, LANES))
        lo_ref[0, rows, :] = jnp.broadcast_to(den, (sub, LANES))
        ao_ref[0, rows, :] = pv


def _update(state, qc, kv, r):
    rows, heads, seq, e = qc.shape
    nh = rows * heads
    tq = min(512, seq)
    sub = min(256, tq)
    first = state is None
    stat = pl.BlockSpec((1, tq, LANES), lambda h, i: (h, i, 0))
    accs = pl.BlockSpec((1, tq, r), lambda h, i: (h, i, 0))
    return pl.pallas_call(
        functools.partial(_block_kernel, r, sub, first),
        grid=(nh, seq // tq),
        in_specs=[pl.BlockSpec((1, tq, e), lambda h, i: (h, i, 0)),
                  pl.BlockSpec((1, seq, e), lambda h, i: (h // heads, 0, 0))] + ([] if first else [stat, stat, accs]),
        out_specs=[stat, stat, accs],
        out_shape=[jax.ShapeDtypeStruct((nh, seq, LANES), F32), jax.ShapeDtypeStruct((nh, seq, LANES), F32),
                   jax.ShapeDtypeStruct((nh, seq, r), F32)],
        compiler_params=pltpu.CompilerParams(dimension_semantics=('arbitrary', 'arbitrary'), vmem_limit_bytes=48 * 2**20),
        cost_estimate=pl.CostEstimate(flops=2 * nh * seq * seq * (e + r), bytes_accessed=nh * seq * (2 * e + 8 * r),
                                      transcendentals=nh * seq * seq),
    )(qc.reshape(nh, seq, e), kv, *(() if first else state))


def _finish(state, w_uv, w_o):
    heads, r, vd = w_uv.shape
    _, den, acc = state
    seq = acc.shape[1]
    den = den[:, :, 0].reshape(-1, heads, seq)
    acc = acc.reshape(-1, heads, seq, r)
    lat = (acc / den[..., None]).astype(BF16)
    o = jnp.einsum('bhqr,hrv->bhqv', lat, w_uv, preferred_element_type=F32).astype(BF16)
    return jnp.einsum('cirw,iwe->cre', o, w_o.reshape(heads, vd, -1), preferred_element_type=F32).astype(BF16)


def _member(idt, first, n):
    e = first + jnp.arange(n, dtype=idt.dtype)
    return jnp.any(idt[..., :, None, :] == e[:, None], axis=-3)


def _ranks(hit):
    t = hit.shape[-1]
    k = jnp.arange(t)
    tri = (k[:, None] < k[None, :]).astype(BF16)
    flat = hit.reshape(-1, t)
    pre = jnp.dot(flat.astype(BF16), tri, preferred_element_type=F32).astype(jnp.int32)
    return jnp.where(flat, pre, -1).reshape(hit.shape)


def _expert(xs, wg, wu, wd):
    hid = jax.nn.silu(jnp.dot(xs, wg, preferred_element_type=F32)) * jnp.dot(xs, wu, preferred_element_type=F32)
    return jnp.dot(hid.astype(BF16), wd, preferred_element_type=F32).astype(BF16)


def _split(w):
    hi = w.astype(BF16)
    r1 = w - hi.astype(F32)
    mid = r1.astype(BF16)
    lo = (r1 - mid.astype(F32)).astype(BF16)
    return hi, mid, lo


def solution(mesh):
    ncp = mesh.shape['cp']
    ngroup = mesh.shape['b'] * ncp
    axes = ('b', 'cp')
    tok = P(('dp', 'b'), 'cp', None)
    rep = P()
    espec = P(('b', 'cp'), None, None)

    def body(x, ids, g_attn, w_q, w_dkv, w_kr, w_uk, w_uv, w_o, g_ffn, w_fg, w_fu, w_fd, g_moe, w_r, w_eg, w_eu, w_ed):
        rows, seq, d = x.shape
        heads, r, _ = w_uv.shape
        top = ids.shape[-1]
        t = rows * seq
        epd = w_eg.shape[0]
        ne = epd * ngroup
        hot = (w_r.shape[1] // top) // 2
        cap = (t + hot - 1) // hot
        i = lax.axis_index('cp')
        me = lax.axis_index('b') * ncp + i
        loc = jnp.arange(seq)
        slots = jnp.arange(cap, dtype=jnp.int32)
        u = _rms(x, g_moe).reshape(t, d)
        idt = ids.reshape(t, top).T
        idall = lax.all_gather(idt, axes, axis=0, tiled=False)
        uall = lax.all_gather(u, axes, axis=0, tiled=False)
        g = jax.nn.softmax(jnp.einsum('td,de->et', u, w_r, preferred_element_type=F32), axis=0)
        hit = _member(idt, 0, g.shape[0])
        sel = jnp.where(hit, g, 0.0)
        gate = sel / jnp.sum(sel, axis=0, keepdims=True)
        rank = _ranks(hit[:ne]).reshape(ngroup, epd, t).transpose(1, 2, 0)
        parts = _split(gate[:ne].reshape(ngroup, epd, t).transpose(1, 2, 0))
        m = jnp.sum(gate[ne:], axis=0)[:, None] * u.astype(F32)
        qc, kv = _prep(x, i * seq + loc, g_attn, w_q, w_dkv, w_kr, w_uk)
        state = _update(None, qc, kv, r)
        perm = [(k, (k + 1) % ncp) for k in range(ncp)]
        early = 1 + (ncp - 1) // 3
        cur = kv

        def attend(step, state, cur):
            cur = lax.ppermute(cur, 'cp', perm)
            state = lax.cond((i - step) % ncp < i,
                             lambda st, kb: tuple(_update(st, qc, kb, r)),
                             lambda st, kb: tuple(st), tuple(state), cur)
            return state, cur

        for step in range(1, min(early, ncp)):
            state, cur = attend(step, state, cur)
        rk = _ranks(_member(idall, me * epd, epd))
        (rk, uall, state, cur) = lax.optimization_barrier((rk, uall, state, cur))

        def chunk(k, src):
            pick = (rk[:, k, None, :] == slots[:, None]).astype(BF16)
            xs = jnp.einsum('sct,std->scd', pick, src, preferred_element_type=F32).astype(BF16)
            out = _expert(xs.reshape(ngroup * cap, d), w_eg[k], w_eu[k], w_ed[k])
            return out.reshape(ngroup, cap, d)

        def weights(k):
            on = rank[k][:, :, None] == slots
            w = jnp.stack([jnp.where(on, part[k][:, :, None].astype(F32), 0.0).astype(BF16) for part in parts])
            return w.reshape(len(parts), t, ngroup * cap)

        def add(m, w, ret):
            part = jnp.einsum('xtp,pd->xtd', w, ret.reshape(ngroup * cap, d), preferred_element_type=F32)
            return m + jnp.sum(part, axis=0)

        rets = []
        for k in range(epd):
            out = chunk(k, uall)
            rets.append(lax.all_to_all(out, axes, 0, 0))
            uall, rk, _ = lax.optimization_barrier((uall, rk, out))
        late = list(range(min(early, ncp), ncp))
        waits = iter(range(epd - 1))
        for step in late:
            k = next(waits, None)
            if k is not None:
                state, rets[k] = lax.optimization_barrier((state, rets[k]))
            state, cur = attend(step, state, cur)
        a = _finish(state, w_uv, w_o)
        y = (x.astype(F32) + a.astype(F32)).astype(BF16).reshape(t, d)
        z = _rms(y, g_ffn)
        for k in waits:
            z, rets[k] = lax.optimization_barrier((z, rets[k]))
        f = _swiglu(z, w_fg, w_fu, w_fd)
        for k in range(epd):
            m = add(m, weights(k), rets[k])
        h = y.astype(F32) + f.astype(F32) + m
        return h.astype(BF16).reshape(rows, seq, d)

    return jax.shard_map(body, mesh=mesh, in_specs=(tok, tok) + (rep,) * 13 + (espec,) * 3, out_specs=tok, check_vma=False)
```
